32 devices in a mesh: head: 2 (over y), outer: 4 (over z), inner: 4 (over x, core).
Axes of the slice: x: 2, y: 2, z: 4, core: 2. Of those that a mesh axis runs over, the one named last changes fastest.
Arguments:
- queries: bfloat16 [1024, 2048], P('outer', ('head', 'inner')), may hold values from -100 to 100
- keys: bfloat16 [1024, 256], P('outer', 'head'), may hold values from -5 to 5
- values: bfloat16 [1024, 256], P('outer', 'head'), may hold values from -6 to 6
- grad_out: bfloat16 [1024, 2048], P('outer', ('head', 'inner')), may hold values from -24 to 24
- hidden_in: bfloat16 [1024, 8192], P('outer', ('head', 'inner')), may hold values from -6 to 6
- adapter_a: bfloat16 [8192, 16], P(('head', 'inner')), may hold values from -0.0625 to 0.0625
- adapter_b: bfloat16 [16, 256], P(None, 'head'), may hold values from -1.5 to 1.5
- block_order: int32 [8], replicated, may hold values from 0 to 7, each once
- doc_ids: int32 [1024], replicated, may hold values from 0 to 3, never falling along the last dimension, each value on 1 to 512 neighbouring positions
Outputs:
- grad_query: bfloat16 [1024, 2048], P('outer', ('head', 'inner'))
- grad_key: bfloat16 [1024, 256], P('outer', 'head')
- grad_value: bfloat16 [1024, 256], P('outer', 'head')
- grad_a: float32 [8192, 16], P(('head', 'inner'))
- grad_b: float32 [16, 256], P(None, 'head')
The draws below stay inside these ranges and needn't reach their ends.
Inputs may be any that keep to these rules, and one draw needn't show every extreme that they name: `block_order`: a permutation of the stored blocks. `doc_ids`: never falling along positions; each document has 1 to 512 positions.
All inputs are finite; a program needn't handle non-finite values.
Results may differ from the reference program's by a relative error of at most 0.024.
Values may be sent and summed in bfloat16 or wider, within the bound.
A program may use at most 64 MiB of HBM per device.

```python
import math
import jax
import jax.numpy as jnp
import numpy as np
from jax import lax

D = 8192
HEAD_DIM = 128
GROUP = 8
RANK = 16
DOCS = 4
TOK_DEV = 256
KV_HEADS = 2
SEQ = 1024
NBLK = 8


def drawn_pair(key):
    base_key = jax.random.fold_in(key, 11)
    key_one, key_two = jax.random.split(base_key, 2)
    query_draw = jax.random.truncated_normal(key_one, -4.5, 4.5, (SEQ, KV_HEADS * GROUP * HEAD_DIM), jnp.float32)
    key_draw = jax.random.truncated_normal(key_two, -4.5, 4.5, (SEQ, KV_HEADS * HEAD_DIM), jnp.float32)
    return (query_draw, key_draw)


def draw_queries(key, part):
    return drawn_pair(key)[0].astype(jnp.bfloat16)


def draw_keys(key, part):
    return drawn_pair(key)[1].astype(jnp.bfloat16)


def shard_levels(key, dims, cuts, smallest, top_value):
    loudness = 1.0
    for dim, parts in cuts:
        steps = jax.random.uniform(jax.random.fold_in(jax.random.fold_in(key, 6), dim), (parts,), jnp.float32, smallest / len(cuts), top_value / len(cuts))
        loudness = loudness * jnp.repeat(jnp.exp(steps), dims[dim] // parts).reshape((-1,) + (1,) * (len(dims) - 1 - dim))
    return loudness


def profile(number_of, total, bound, lean):
    portions = [(1 << 20) // math.isqrt(grade ** lean) + 1 for grade in range(2, number_of + 1)]
    rest, holding = total - bound - (number_of - 1), [1] * (number_of - 1)
    while rest > 0:
        movable = [i for i in range(number_of - 1) if holding[i] < bound]
        pool, left = sum([portions[i] for i in movable]), rest
        for i in movable:
            addition = min(bound - holding[i], max(1, left * portions[i] // pool), rest)
            holding[i] = holding[i] + addition
            rest = rest - addition
    return np.array([bound] + holding)


def ragged(rng, amount, total, bound, lean):
    if amount == 2:
        one = jax.random.randint(rng, (), max(1, total - bound), min(bound, total - 1) + 1)
        return jnp.stack([one, total - one])
    sizes = jnp.asarray(profile(amount, total, bound, lean), jnp.int32)
    couples = (amount - 1) // 2
    source_of, taker = sizes[1:1 + 2 * couples:2], sizes[2:2 + 2 * couples:2]
    margin = jnp.minimum(source_of - 1, bound - taker)
    shifted = jax.random.randint(jax.random.fold_in(rng, 1), (couples,), 0, 1 << 20) % (margin + 1)
    sizes = sizes.at[1:1 + 2 * couples:2].set(source_of - shifted).at[2:2 + 2 * couples:2].set(taker + shifted)
    return sizes[jax.random.permutation(jax.random.fold_in(rng, 2), amount)]


def noise(stream_key, extent, width, limit, cuts=(), kind=jnp.bfloat16):
    factor_of = shard_levels(stream_key, extent, cuts, -0.22, 0.18) if cuts else 1.0
    values = jax.random.normal(stream_key, extent, jnp.float32) * width * factor_of
    return jnp.minimum(jnp.maximum(values, -limit), limit).astype(kind)


def setup_inputs(seed: int = 0) -> dict:
    streams_of = jax.random.split(jax.random.key(seed), 10)
    return {
        "queries": draw_queries(jax.random.fold_in(streams_of[9], 71), 0),
        "keys": draw_keys(jax.random.fold_in(streams_of[9], 71), 0),
        "values": noise(streams_of[2], (SEQ, KV_HEADS * HEAD_DIM), 1.0, 6.0, ((0, 4), (1, 2))),
        "grad_out": noise(streams_of[3], (SEQ, KV_HEADS * GROUP * HEAD_DIM), 4.0, 24.0, ((0, 4), (1, 8))),
        "hidden_in": noise(streams_of[4], (SEQ, D), 1.0, 6.0, ((0, 4), (1, 8))),
        "adapter_a": noise(streams_of[5], (D, RANK), D ** -0.5, 0.0625, ((0, 8),)),
        "adapter_b": noise(streams_of[6], (RANK, KV_HEADS * HEAD_DIM), RANK ** -0.5, 1.5, ((1, 2),)),
        "block_order": jax.random.permutation(streams_of[7], NBLK).astype(jnp.int32),
        "doc_ids": jnp.searchsorted(jnp.cumsum(ragged(streams_of[8], DOCS, SEQ, SEQ // 2, 2)), jnp.arange(SEQ), side="right").astype(jnp.int32),
    }


NEGATIVE = -1.0e30


def rounded(values_in):
    return lax.optimization_barrier(values_in.astype(jnp.bfloat16)).astype(jnp.float32)


def head_pass(query_head, key_head, value_head, grad_head, places, owners):
    total_rows = key_head.shape[0]
    length = min(512, total_rows)
    scaling = HEAD_DIM ** -0.5
    keys_wide = key_head.astype(jnp.float32)
    values_wide = value_head.astype(jnp.float32)

    def block_step(carried, first_row):
        grad_key, grad_value = carried
        query_blk = lax.dynamic_slice_in_dim(query_head, first_row, length, 0).astype(jnp.float32)
        grad_blk = lax.dynamic_slice_in_dim(grad_head, first_row, length, 0).astype(jnp.float32)
        q_places = lax.dynamic_slice_in_dim(places, first_row, length, 0)
        q_owners = lax.dynamic_slice_in_dim(owners, first_row, length, 0)
        masked = (places[None, :] <= q_places[:, None]) & (owners[None, :] == q_owners[:, None])
        scores = jnp.einsum("tgd,sd->gts", query_blk, keys_wide) * scaling
        scores = jnp.where(masked[None], scores, NEGATIVE)
        peak_score = jnp.max(scores, axis=-1)
        weights = jnp.where(masked[None], jnp.exp(scores - peak_score[..., None]), 0.0)
        totals = jnp.sum(weights, axis=-1)
        output = jnp.einsum("gts,sd->gtd", rounded(weights), values_wide) / totals[..., None]
        lse_rows = peak_score + jnp.log(totals)
        delta_rows = jnp.sum(output * jnp.transpose(grad_blk, (1, 0, 2)), axis=-1)
        prob_tile = jnp.where(masked[None], jnp.exp(scores - lse_rows[..., None]), 0.0)
        grad_value = grad_value + jnp.einsum("gts,tgd->sd", rounded(prob_tile), grad_blk)
        dot_tile = jnp.einsum("tgd,sd->gts", grad_blk, values_wide)
        slopes = rounded(prob_tile * (dot_tile - delta_rows[..., None]))
        grad_query = jnp.einsum("gts,sd->tgd", slopes, keys_wide) * scaling
        grad_key = grad_key + jnp.einsum("gts,tgd->sd", slopes, query_blk)
        return (grad_key, grad_value), grad_query.astype(jnp.bfloat16)

    starts = jnp.arange(0, total_rows, length, dtype=jnp.int32)
    empty_rows = jnp.zeros((total_rows, HEAD_DIM), jnp.float32)
    (grad_key, grad_value), grad_query = lax.scan(block_step, (empty_rows, empty_rows), starts)
    grad_query = grad_query.reshape(total_rows, GROUP, HEAD_DIM)
    return grad_query, (grad_key * scaling).astype(jnp.bfloat16), grad_value.astype(jnp.bfloat16)


def reference(queries, keys, values, grad_out, hidden_in, adapter_a, adapter_b, block_order, doc_ids):
    total_rows = queries.shape[0]
    half_rows = TOK_DEV // 2
    kv_heads = keys.shape[1] // HEAD_DIM
    places = (block_order[:, None] * half_rows + jnp.arange(half_rows, dtype=jnp.int32)[None, :]).reshape(-1).astype(jnp.int32)
    owners = jnp.take(doc_ids, places).astype(jnp.int32)
    query_heads = jnp.transpose(queries.reshape(total_rows, kv_heads, GROUP, HEAD_DIM), (1, 0, 2, 3))
    grad_heads = jnp.transpose(grad_out.reshape(total_rows, kv_heads, GROUP, HEAD_DIM), (1, 0, 2, 3))
    key_heads = jnp.transpose(keys.reshape(total_rows, kv_heads, HEAD_DIM), (1, 0, 2))
    value_heads = jnp.transpose(values.reshape(total_rows, kv_heads, HEAD_DIM), (1, 0, 2))

    def one_head(packed):
        return head_pass(packed[0], packed[1], packed[2], packed[3], places, owners)

    grad_q, grad_k, grad_v = lax.map(one_head, (query_heads, key_heads, value_heads, grad_heads))
    grad_query = jnp.transpose(grad_q, (1, 0, 2, 3)).reshape(total_rows, -1)
    grad_key = jnp.transpose(grad_k, (1, 0, 2)).reshape(total_rows, -1)
    grad_value = jnp.transpose(grad_v, (1, 0, 2)).reshape(total_rows, -1)
    low_rank = jnp.dot(hidden_in, adapter_a, preferred_element_type=jnp.float32).astype(jnp.bfloat16)
    back_rank = lax.dot_general(grad_key, adapter_b, (((1,), (1,)), ((), ())), preferred_element_type=jnp.float32).astype(jnp.bfloat16)
    grad_a = lax.dot_general(hidden_in, back_rank, (((0,), (0,)), ((), ())), preferred_element_type=jnp.float32)
    grad_b = lax.dot_general(low_rank, grad_key, (((0,), (0,)), ((), ())), preferred_element_type=jnp.float32)
    return grad_query, grad_key, grad_value, grad_a, grad_b
```

```python
import functools

import jax
import jax.numpy as jnp
from jax import lax
from jax.experimental import pallas as pl
from jax.experimental.pallas import tpu as pltpu
from jax.sharding import PartitionSpec as P

HEAD_DIM = 128
NEGATIVE = -1e30
MESH = pl.DeviceIdType.MESH
NT = (((1,), (1,)), ((), ()))
NN = (((1,), (0,)), ((), ()))
TN = (((0,), (0,)), ((), ()))


def mm(a, b, dims):
    return lax.dot_general(a, b, dims, preferred_element_type=jnp.float32)


def kernel(
    sizes,
    order_ref, docs_ref, q_hbm, k_hbm, v_hbm, g_hbm, hid_hbm, at_ref, b_ref,
    dq_ref, dk_ref, dv_ref, ga_ref, gb_ref,
    q_ref, g_ref, hid_ref, kv, st, dpt, dq_acc,
    low_out, low_in, rs1_out, rs1_in, rs2_out, rs2_in, fin, gbq, back_in, part_a, part_b,
    load_sem, kv_send, kv_recv, fw_send, low_send, low_recv,
    rs1_send, rs1_recv, rs2_send, rs2_recv, fin_send, fin_recv,
    gbq_send, gbq_recv, back_send, back_recv,
    pa_send, pa_recv, pb_send, pb_recv,
):
    nh, no, ni, heads = sizes
    h, o, i = lax.axis_index("head"), lax.axis_index("outer"), lax.axis_index("inner")
    rows = q_ref.shape[0]
    half = rows // 2
    part = rows // ni
    plane = nh * ni
    me = h * ni + i
    scaling = HEAD_DIM ** -0.5

    def at_outer(t):
        return lax.rem(o + t, no)

    def at_inner(t):
        return lax.rem(i + t, ni)

    def at_plane(t):
        return lax.rem(me + t, plane)

    def remote(src, dst, send, recv, dev):
        return pltpu.make_async_remote_copy(
            src_ref=src, dst_ref=dst, send_sem=send, recv_sem=recv, device_id=dev,
            device_id_type=MESH,
        )

    def plane_dev(p):
        return (p // ni, o, lax.rem(p, ni))

    kv_loads = []
    for j in range(ni):
        for which, src in enumerate((k_hbm, v_hbm)):
            kv_loads.append(
                pltpu.make_async_copy(
                    src.at[pl.ds(j * part, part)], kv.at[o, j, which],
                    load_sem.at[3 + 2 * j + which],
                )
            )
    q_load = pltpu.make_async_copy(q_hbm, q_ref, load_sem.at[0])
    g_load = pltpu.make_async_copy(g_hbm, g_ref, load_sem.at[1])
    hid_load = pltpu.make_async_copy(hid_hbm, hid_ref, load_sem.at[2])
    for copy in kv_loads + [hid_load, q_load, g_load]:
        copy.start()

    barrier = pltpu.get_barrier_semaphore()
    for t in range(1, no):
        pl.semaphore_signal(barrier, inc=1, device_id=(h, at_outer(t), i), device_id_type=MESH)
    for t in range(1, plane):
        pl.semaphore_signal(barrier, inc=1, device_id=plane_dev(at_plane(t)), device_id_type=MESH)
    pl.semaphore_wait(barrier, no - 1 + plane - 1)

    for copy in kv_loads:
        copy.wait()

    def kv_copy(t):
        return remote(kv.at[o, i], kv.at[o, i], kv_send.at[t], kv_recv.at[o, i],
                      (h, at_outer(t), i))

    def slot_wait(src, j):
        remote(kv.at[src, j], kv.at[src, j], kv_send.at[0], kv_recv.at[src, j],
               (h, at_outer(1), i)).wait_recv()

    def fw_copy(src, t, k):
        return remote(kv.at[src, i], kv.at[src, i], fw_send.at[t, k], kv_recv.at[src, i],
                      (h, o, at_inner(k)))

    for t in range(1, no):
        kv_copy(t).start()

    hid_load.wait()
    for j in range(ni):
        low_out[j] = mm(at_ref[...], hid_ref[j * part:(j + 1) * part, :], NT)
    low_in[me] = low_out[i]

    def low_copy(t):
        p = at_plane(t)
        return remote(low_out.at[lax.rem(p, ni)], low_in.at[me], low_send.at[t],
                      low_recv.at[me], plane_dev(p))

    for t in range(1, plane):
        low_copy(t).start()

    q_load.wait()
    g_load.wait()

    def row_meta(block):
        idx = order_ref[block]
        doc = docs_ref[pl.ds(idx, 1), :].astype(jnp.float32)
        return doc, idx * half

    lanes = lax.broadcasted_iota(jnp.int32, (1, half), 1)
    sublanes = lax.broadcasted_iota(jnp.int32, (half, rows), 0)
    qm = [row_meta(2 * o + b) for b in range(2)]
    q_doc = jnp.concatenate([m[0] for m in qm], 1)
    q_pos = jnp.concatenate([m[1] + lanes for m in qm], 1)

    def head_cols(x):
        return slice(x * HEAD_DIM, (x + 1) * HEAD_DIM)

    def block_scores(src, t, peaks):
        key_rows = kv[src, :, 0].reshape(rows, HEAD_DIM)
        val_rows = kv[src, :, 1].reshape(rows, HEAD_DIM)
        docs, poss = [], []
        for b in range(2):
            doc, first = row_meta(2 * src + b)
            wide = jnp.transpose(jnp.broadcast_to(doc, (half, half)))
            docs.append(jnp.concatenate([wide] * (rows // half), 1))
            poss.append(first + sublanes)
        seen = (jnp.concatenate(docs, 0) == q_doc) & (jnp.concatenate(poss, 0) <= q_pos)
        out = []
        for x in range(heads):
            s = mm(key_rows, q_ref[:, head_cols(x)], NT) * scaling
            s = jnp.where(seen, s, NEGATIVE)
            st[t, x] = s
            out.append(jnp.maximum(peaks[x], jnp.max(s, axis=0, keepdims=True)))
            dpt[t, x] = mm(val_rows, g_ref[:, head_cols(x)], NT)
        return tuple(out)

    peaks = tuple(jnp.full((1, rows), NEGATIVE, jnp.float32) for _ in range(heads))
    peaks = block_scores(o, 0, peaks)

    def forward(t):
        src = lax.rem(o - t + no, no)
        slot_wait(src, i)
        for k in range(1, ni):
            fw_copy(src, t, k).start()

    forward(1)

    def gather_step(t, peaks):
        @pl.when(t < no - 1)
        def _():
            forward(t + 1)

        src = lax.rem(o - t + no, no)
        for k in range(1, ni):
            slot_wait(src, at_inner(k))
        return block_scores(src, t, peaks)

    peaks = lax.fori_loop(1, no, gather_step, peaks)

    zero = jnp.zeros((1, rows), jnp.float32)

    def weigh_step(t, carried):
        out = []
        for x in range(heads):
            total, dot = carried[x]
            w = jnp.exp(st[t, x] - peaks[x])
            st[t, x] = w
            out.append((total + jnp.sum(w, axis=0, keepdims=True),
                        dot + jnp.sum(w * dpt[t, x], axis=0, keepdims=True)))
        return tuple(out)

    sums = lax.fori_loop(0, no, weigh_step, tuple((zero, zero) for _ in range(heads)))
    inv = [1.0 / total for total, _ in sums]
    delta = [dot * r for (_, dot), r in zip(sums, inv)]

    dq_acc[...] = jnp.zeros_like(dq_acc)

    def rs1_copy(src, k):
        return remote(rs1_out.at[src, at_inner(k)], rs1_in.at[src, i], rs1_send.at[src, k],
                      rs1_recv.at[src, i], (h, o, at_inner(k)))

    def grad_step(n, _):
        t = lax.rem(n + 1, no)
        src = lax.rem(o - t + no, no)
        key_rows = kv[src, :, 0].reshape(rows, HEAD_DIM)
        dk = jnp.zeros((rows, HEAD_DIM), jnp.float32)
        dv = jnp.zeros((rows, HEAD_DIM), jnp.float32)
        for x in range(heads):
            p = st[t, x] * inv[x]
            ds = (p * (dpt[t, x] - delta[x])).astype(jnp.bfloat16)
            dv += mm(p.astype(jnp.bfloat16), g_ref[:, head_cols(x)], NN)
            dk += mm(ds, q_ref[:, head_cols(x)], NN)
            dq_acc[:, head_cols(x)] += mm(ds, key_rows, TN)
        rs1_out[src, :, 0] = dk.astype(jnp.bfloat16).reshape(ni, part, HEAD_DIM)
        rs1_out[src, :, 1] = dv.astype(jnp.bfloat16).reshape(ni, part, HEAD_DIM)
        for k in range(1, ni):
            rs1_copy(src, k).start()
        return 0

    lax.fori_loop(0, no, grad_step, 0)
    dq_ref[...] = (dq_acc[...] * scaling).astype(jnp.bfloat16)

    def inner_sum(src):
        acc = rs1_out[src, i].astype(jnp.float32)
        for k in range(1, ni):
            j = at_inner(k)
            remote(rs1_in.at[src, j], rs1_in.at[src, j], rs1_send.at[src, k],
                   rs1_recv.at[src, j], (h, o, j)).wait_recv()
            acc = acc + rs1_in[src, j].astype(jnp.float32)
        return acc

    def rs2_copy(t):
        dst = lax.rem(o - t + no, no)
        return remote(rs2_out.at[t], rs2_in.at[o], rs2_send.at[t], rs2_recv.at[o], (h, dst, i))

    def home_step(t, _):
        rs2_out[t] = inner_sum(lax.rem(o - t + no, no)).astype(jnp.bfloat16)
        rs2_copy(t).start()
        return 0

    lax.fori_loop(1, no, home_step, 0)
    acc = inner_sum(o)
    for t in range(1, no):
        src = at_outer(t)
        remote(rs2_out.at[t], rs2_in.at[src], rs2_send.at[t], rs2_recv.at[src],
               (h, src, i)).wait_recv()
        acc = acc + rs2_in[src].astype(jnp.float32)
    dk_part = (acc[0] * scaling).astype(jnp.bfloat16)
    dv_part = acc[1].astype(jnp.bfloat16)
    back_in[me] = mm(b_ref[...], dk_part, NT)

    def back_copy(t):
        return remote(back_in.at[me], back_in.at[me], back_send.at[t], back_recv.at[me],
                      plane_dev(at_plane(t)))

    for t in range(1, plane):
        back_copy(t).start()
    fin[i, 0] = dk_part
    fin[i, 1] = dv_part

    low = low_in[me]
    for t in range(1, plane):
        p = at_plane(t)
        remote(low_out.at[0], low_in.at[p], low_send.at[t], low_recv.at[p],
               plane_dev(p)).wait_recv()
        low = low + low_in[p]
    gbq[i] = mm(low.astype(jnp.bfloat16), dk_part, NN)

    def fin_copy(k):
        return remote(fin.at[i], fin.at[i], fin_send.at[k], fin_recv.at[i], (h, o, at_inner(k)))

    def gbq_copy(k):
        return remote(gbq.at[i], gbq.at[i], gbq_send.at[k], gbq_recv.at[i], (h, o, at_inner(k)))

    for k in range(1, ni):
        gbq_copy(k).start()
        fin_copy(k).start()

    for t in range(1, plane):
        p = at_plane(t)
        remote(back_in.at[p], back_in.at[p], back_send.at[t], back_recv.at[p],
               plane_dev(p)).wait_recv()
    acc_a = jnp.zeros(ga_ref.shape, jnp.float32)
    for j in range(ni):
        back = back_in[j]
        for y in range(1, nh):
            back = back + back_in[y * ni + j]
        acc_a += mm(back.astype(jnp.bfloat16), hid_ref[j * part:(j + 1) * part, :], NN)
    part_a[o] = acc_a.astype(jnp.bfloat16)

    def pa_copy(t):
        return remote(part_a.at[o], part_a.at[o], pa_send.at[t], pa_recv.at[o],
                      (h, at_outer(t), i))

    def pb_copy(t):
        return remote(part_b.at[o], part_b.at[o], pb_send.at[t], pb_recv.at[o],
                      (h, at_outer(t), i))

    for t in range(1, no):
        pa_copy(t).start()

    for k in range(1, ni):
        j = at_inner(k)
        remote(gbq.at[j], gbq.at[j], gbq_send.at[k], gbq_recv.at[j], (h, o, j)).wait_recv()
    acc_b = gbq[0]
    for j in range(1, ni):
        acc_b = acc_b + gbq[j]
    part_b[o] = acc_b.astype(jnp.bfloat16)
    for t in range(1, no):
        pb_copy(t).start()

    for k in range(1, ni):
        j = at_inner(k)
        remote(fin.at[j], fin.at[j], fin_send.at[k], fin_recv.at[j], (h, o, j)).wait_recv()
    dk_ref[...] = fin[:, 0].reshape(rows, HEAD_DIM)
    dv_ref[...] = fin[:, 1].reshape(rows, HEAD_DIM)

    for t in range(1, no):
        kv_copy(t).wait_send()
        rs2_copy(t).wait_send()
        for k in range(1, ni):
            fw_copy(lax.rem(o - t + no, no), t, k).wait_send()
    for t in range(1, plane):
        low_copy(t).wait_send()
        back_copy(t).wait_send()
    for src in range(no):
        for k in range(1, ni):
            rs1_copy(src, k).wait_send()
    for k in range(1, ni):
        fin_copy(k).wait_send()
        gbq_copy(k).wait_send()

    for t in range(1, no):
        src = at_outer(t)
        remote(part_a.at[src], part_a.at[src], pa_send.at[t], pa_recv.at[src],
               (h, src, i)).wait_recv()
        remote(part_b.at[src], part_b.at[src], pb_send.at[t], pb_recv.at[src],
               (h, src, i)).wait_recv()
    total_a = part_a[0].astype(jnp.float32)
    total_b = part_b[0].astype(jnp.float32)
    for src in range(1, no):
        total_a += part_a[src].astype(jnp.float32)
        total_b += part_b[src].astype(jnp.float32)
    ga_ref[...] = total_a
    gb_ref[...] = total_b
    for t in range(1, no):
        pa_copy(t).wait_send()
        pb_copy(t).wait_send()


def on_device(
    sizes, queries, keys, values, grad_out, hidden_in, adapter_a, adapter_b, block_order, doc_ids
):
    nh, no, ni = sizes
    rows = queries.shape[0]
    half = rows // 2
    part = rows // ni
    width = hidden_in.shape[1]
    rank = adapter_a.shape[1]
    heads = queries.shape[1] // HEAD_DIM
    plane = nh * ni
    docs = doc_ids.reshape(-1, half)
    bf, f32 = jnp.bfloat16, jnp.float32
    dma = pltpu.SemaphoreType.DMA
    vmem = pl.BlockSpec(memory_space=pltpu.VMEM)
    hbm = pl.BlockSpec(memory_space=pl.ANY)
    share = (2, part, HEAD_DIM)
    grad_query, grad_key, grad_value, grad_a, grad_b = pl.pallas_call(
        functools.partial(kernel, (nh, no, ni, heads)),
        out_shape=(
            jax.ShapeDtypeStruct(queries.shape, bf),
            jax.ShapeDtypeStruct(keys.shape, bf),
            jax.ShapeDtypeStruct(values.shape, bf),
            jax.ShapeDtypeStruct((rank, width), f32),
            jax.ShapeDtypeStruct((rank, HEAD_DIM), f32),
        ),
        in_specs=[
            pl.BlockSpec(memory_space=pltpu.SMEM), vmem, hbm, hbm, hbm, hbm, hbm, vmem, vmem,
        ],
        out_specs=(vmem,) * 5,
        scratch_shapes=[
            pltpu.VMEM(queries.shape, bf),
            pltpu.VMEM(queries.shape, bf),
            pltpu.VMEM((rows, width), bf),
            pltpu.VMEM((no, ni) + share, bf),
            pltpu.VMEM((no, heads, rows, rows), f32),
            pltpu.VMEM((no, heads, rows, rows), f32),
            pltpu.VMEM(queries.shape, f32),
            pltpu.VMEM((ni, rank, part), f32),
            pltpu.VMEM((plane, rank, part), f32),
            pltpu.VMEM((no, ni) + share, bf),
            pltpu.VMEM((no, ni) + share, bf),
            pltpu.VMEM((no,) + share, bf),
            pltpu.VMEM((no,) + share, bf),
            pltpu.VMEM((ni,) + share, bf),
            pltpu.VMEM((ni, rank, HEAD_DIM), f32),
            pltpu.VMEM((plane, rank, part), f32),
            pltpu.VMEM((no, rank, width), bf),
            pltpu.VMEM((no, rank, HEAD_DIM), bf),
            dma((3 + 2 * ni,)),
            dma((no,)), dma((no, ni)), dma((no, ni)),
            dma((plane,)), dma((plane,)),
            dma((no, ni)), dma((no, ni)),
            dma((no,)), dma((no,)),
            dma((ni,)), dma((ni,)),
            dma((ni,)), dma((ni,)),
            dma((plane,)), dma((plane,)),
            dma((no,)), dma((no,)),
            dma((no,)), dma((no,)),
        ],
        compiler_params=pltpu.CompilerParams(
            collective_id=0, has_side_effects=True, vmem_limit_bytes=60 * 1024 * 1024
        ),
    )(block_order, docs, queries, keys, values, grad_out, hidden_in, adapter_a.T, adapter_b)
    return grad_query, grad_key, grad_value, grad_a.T, grad_b


def solution(mesh):
    sizes = tuple(mesh.shape[name] for name in ("head", "outer", "inner"))
    in_specs = (
        P("outer", ("head", "inner")),
        P("outer", "head"),
        P("outer", "head"),
        P("outer", ("head", "inner")),
        P("outer", ("head", "inner")),
        P(("head", "inner"), None),
        P(None, "head"),
        P(),
        P(),
    )
    out_specs = (
        P("outer", ("head", "inner")),
        P("outer", "head"),
        P("outer", "head"),
        P(("head", "inner"), None),
        P(None, "head"),
    )
    return jax.shard_map(
        functools.partial(on_device, sizes),
        mesh=mesh, in_specs=in_specs, out_specs=out_specs, check_vma=False,
    )
```

```python
import functools

import jax
import jax.numpy as jnp
from jax import lax
from jax.experimental import pallas as pl
from jax.experimental.pallas import tpu as pltpu
from jax.sharding import PartitionSpec as P

HEAD_DIM = 128
NEGATIVE = -1e30
MESH = pl.DeviceIdType.MESH
NT = (((1,), (1,)), ((), ()))
NN = (((1,), (0,)), ((), ()))
TN = (((0,), (0,)), ((), ()))


def mm(a, b, dims):
    return lax.dot_general(a, b, dims, preferred_element_type=jnp.float32)


def kernel(
    sizes,
    order_ref, docs_ref, q_hbm, k_hbm, v_hbm, g_hbm, hid_hbm, at_ref, b_ref,
    dq_ref, dk_ref, dv_ref, ga_ref, gb_ref,
    q_ref, g_ref, hid_ref, kv, st, dpt, dq_acc,
    low_out, low_in, low_all, rs1_out, rs1_in, rs2_out, rs2_in, fin, gbq, zb_out, zb_in, back_in,
    part_a, part_b,
    load_sem, kv_send, kv_recv, fx_send, fs_send, low_send, low_recv, la_send, la_recv,
    rs1_send, rs1_recv, rs2_send, rs2_recv, fin_send, fin_recv,
    gbq_send, gbq_recv, zb_send, zb_recv, back_send, back_recv,
    pa_send, pa_recv, pb_send, pb_recv,
):
    nh, no, ni, heads = sizes
    h, o, i = lax.axis_index("head"), lax.axis_index("outer"), lax.axis_index("inner")
    rows = q_ref.shape[0]
    half = rows // 2
    part = rows // ni
    plane = nh * ni
    me = h * ni + i
    scaling = HEAD_DIM ** -0.5

    def at_outer(t):
        return lax.rem(o + t, no)

    def at_inner(t):
        return lax.rem(i + t, ni)

    def at_plane(t):
        return lax.rem(me + t, plane)

    def remote(src, dst, send, recv, dev):
        return pltpu.make_async_remote_copy(
            src_ref=src, dst_ref=dst, send_sem=send, recv_sem=recv, device_id=dev,
            device_id_type=MESH,
        )

    def plane_dev(p):
        return (p // ni, o, lax.rem(p, ni))

    kv_loads = []
    for j in range(ni):
        for which, src in enumerate((k_hbm, v_hbm)):
            kv_loads.append(
                pltpu.make_async_copy(
                    src.at[pl.ds(j * part, part)], kv.at[o, j, which],
                    load_sem.at[3 + 2 * j + which],
                )
            )
    q_load = pltpu.make_async_copy(q_hbm, q_ref, load_sem.at[0])
    g_load = pltpu.make_async_copy(g_hbm, g_ref, load_sem.at[1])
    hid_load = pltpu.make_async_copy(hid_hbm, hid_ref, load_sem.at[2])
    for copy in kv_loads + [hid_load, q_load, g_load]:
        copy.start()

    barrier = pltpu.get_barrier_semaphore()
    for t in range(1, no):
        pl.semaphore_signal(barrier, inc=1, device_id=(h, at_outer(t), i), device_id_type=MESH)
    for t in range(1, plane):
        pl.semaphore_signal(barrier, inc=1, device_id=plane_dev(at_plane(t)), device_id_type=MESH)
    pl.semaphore_wait(barrier, no - 1 + plane - 1)

    for copy in kv_loads:
        copy.wait()

    def kv_copy(t):
        return remote(kv.at[o, i], kv.at[o, i], kv_send.at[t], kv_recv.at[o, i],
                      (h, at_outer(t), i))

    def slot_wait(src, j):
        remote(kv.at[src, j], kv.at[src, j], kv_send.at[0], kv_recv.at[src, j],
               (h, at_outer(1), i)).wait_recv()

    sibling = i + 1 - 2 * lax.rem(i, 2)

    def cross(k):
        return at_inner(2 * k)

    def cross_copy(src, t, k):
        return remote(kv.at[src, i], kv.at[src, i], fx_send.at[t, k], kv_recv.at[src, i],
                      (h, o, cross(k)))

    def sibling_copy(src, t, k):
        j = cross(k)
        return remote(kv.at[src, j], kv.at[src, j], fs_send.at[t, k], kv_recv.at[src, j],
                      (h, o, sibling))

    for t in range(1, no):
        kv_copy(t).start()

    hid_load.wait()
    for j in range(ni):
        low_out[j] = mm(at_ref[...], hid_ref[j * part:(j + 1) * part, :], NT)
    low_in[me] = low_out[i]

    def low_copy(t):
        p = at_plane(t)
        return remote(low_out.at[lax.rem(p, ni)], low_in.at[me], low_send.at[t],
                      low_recv.at[me], plane_dev(p))

    for t in range(1, plane):
        low_copy(t).start()

    q_load.wait()
    g_load.wait()

    def row_meta(block):
        idx = order_ref[block]
        doc = docs_ref[pl.ds(idx, 1), :].astype(jnp.float32)
        return doc, idx * half

    lanes = lax.broadcasted_iota(jnp.int32, (1, half), 1)
    sublanes = lax.broadcasted_iota(jnp.int32, (half, rows), 0)
    qm = [row_meta(2 * o + b) for b in range(2)]
    q_doc = jnp.concatenate([m[0] for m in qm], 1)
    q_pos = jnp.concatenate([m[1] + lanes for m in qm], 1)

    def head_cols(x):
        return slice(x * HEAD_DIM, (x + 1) * HEAD_DIM)

    def block_scores(src, t, peaks):
        key_rows = kv[src, :, 0].reshape(rows, HEAD_DIM)
        val_rows = kv[src, :, 1].reshape(rows, HEAD_DIM)
        docs, poss = [], []
        for b in range(2):
            doc, first = row_meta(2 * src + b)
            wide = jnp.transpose(jnp.broadcast_to(doc, (half, half)))
            docs.append(jnp.concatenate([wide] * (rows // half), 1))
            poss.append(first + sublanes)
        seen = (jnp.concatenate(docs, 0) == q_doc) & (jnp.concatenate(poss, 0) <= q_pos)
        out = []
        for x in range(heads):
            s = mm(key_rows, q_ref[:, head_cols(x)], NT) * scaling
            s = jnp.where(seen, s, NEGATIVE)
            st[t, x] = s
            out.append(jnp.maximum(peaks[x], jnp.max(s, axis=0, keepdims=True)))
            dpt[t, x] = mm(val_rows, g_ref[:, head_cols(x)], NT)
        return tuple(out)

    peaks = tuple(jnp.full((1, rows), NEGATIVE, jnp.float32) for _ in range(heads))
    peaks = block_scores(o, 0, peaks)

    def forward(t):
        src = lax.rem(o - t + no, no)
        slot_wait(src, i)
        for k in range(1, ni // 2):
            cross_copy(src, t, k).start()
        sibling_copy(src, t, 0).start()

    forward(1)

    def gather_step(t, peaks):
        @pl.when(t < no - 1)
        def _():
            forward(t + 1)

        src = lax.rem(o - t + no, no)
        for k in range(1, ni // 2):
            slot_wait(src, cross(k))
            sibling_copy(src, t, k).start()
        for k in range(ni // 2):
            slot_wait(src, lax.rem(sibling + 2 * k, ni))
        return block_scores(src, t, peaks)

    peaks = lax.fori_loop(1, no, gather_step, peaks)

    low = low_in[me]
    for t in range(1, plane):
        p = at_plane(t)
        remote(low_out.at[0], low_in.at[p], low_send.at[t], low_recv.at[p],
               plane_dev(p)).wait_recv()
        low = low + low_in[p]
    low_all[o] = low.astype(jnp.bfloat16)

    def la_copy(t):
        return remote(low_all.at[o], low_all.at[o], la_send.at[t], la_recv.at[o],
                      (h, at_outer(t), i))

    for t in range(1, no):
        la_copy(t).start()

    zero = jnp.zeros((1, rows), jnp.float32)

    def weigh_step(t, carried):
        out = []
        for x in range(heads):
            total, dot = carried[x]
            w = jnp.exp(st[t, x] - peaks[x])
            st[t, x] = w
            out.append((total + jnp.sum(w, axis=0, keepdims=True),
                        dot + jnp.sum(w * dpt[t, x], axis=0, keepdims=True)))
        return tuple(out)

    sums = lax.fori_loop(0, no, weigh_step, tuple((zero, zero) for _ in range(heads)))
    inv = [1.0 / total for total, _ in sums]
    delta = [dot * r for (_, dot), r in zip(sums, inv)]

    dq_acc[...] = jnp.zeros_like(dq_acc)

    def rs1_copy(src, k):
        return remote(rs1_out.at[src, at_inner(k)], rs1_in.at[src, i], rs1_send.at[src, k],
                      rs1_recv.at[src, i], (h, o, at_inner(k)))

    def zb_copy(t):
        dst = lax.rem(o - t + no, no)
        return remote(zb_out.at[t], zb_in.at[o], zb_send.at[t], zb_recv.at[o], (h, dst, i))

    def grad_step(n, _):
        t = lax.rem(n + 1, no)
        src = lax.rem(o - t + no, no)
        key_rows = kv[src, :, 0].reshape(rows, HEAD_DIM)
        dk = jnp.zeros((rows, HEAD_DIM), jnp.float32)
        dv = jnp.zeros((rows, HEAD_DIM), jnp.float32)
        for x in range(heads):
            p = st[t, x] * inv[x]
            ds = (p * (dpt[t, x] - delta[x])).astype(jnp.bfloat16)
            dv += mm(p.astype(jnp.bfloat16), g_ref[:, head_cols(x)], NN)
            dk += mm(ds, q_ref[:, head_cols(x)], NN)
            dq_acc[:, head_cols(x)] += mm(ds, key_rows, TN)
        rs1_out[src, :, 0] = dk.astype(jnp.bfloat16).reshape(ni, part, HEAD_DIM)
        rs1_out[src, :, 1] = dv.astype(jnp.bfloat16).reshape(ni, part, HEAD_DIM)
        for k in range(1, ni):
            rs1_copy(src, k).start()
        back = mm(b_ref[...], dk.astype(jnp.bfloat16), NT) * scaling
        zb_out[t] = back.astype(jnp.bfloat16)

        @pl.when(t > 0)
        def _():
            zb_copy(t).start()

        return 0

    lax.fori_loop(0, no, grad_step, 0)
    dq_ref[...] = (dq_acc[...] * scaling).astype(jnp.bfloat16)

    acc = zb_out[0].astype(jnp.float32)
    for t in range(1, no):
        src = at_outer(t)
        remote(zb_out.at[t], zb_in.at[src], zb_send.at[t], zb_recv.at[src],
               (h, src, i)).wait_recv()
        acc = acc + zb_in[src].astype(jnp.float32)
    back_in[me] = acc.astype(jnp.bfloat16)

    def back_copy(t):
        return remote(back_in.at[me], back_in.at[me], back_send.at[t], back_recv.at[me],
                      plane_dev(at_plane(t)))

    for t in range(1, plane):
        back_copy(t).start()

    for t in range(1, no):
        src = at_outer(t)
        remote(low_all.at[src], low_all.at[src], la_send.at[t], la_recv.at[src],
               (h, src, i)).wait_recv()

    def inner_sum(src):
        acc = rs1_out[src, i].astype(jnp.float32)
        for k in range(1, ni):
            j = at_inner(k)
            remote(rs1_in.at[src, j], rs1_in.at[src, j], rs1_send.at[src, k],
                   rs1_recv.at[src, j], (h, o, j)).wait_recv()
            acc = acc + rs1_in[src, j].astype(jnp.float32)
        return acc

    def rs2_copy(t):
        dst = lax.rem(o - t + no, no)
        return remote(rs2_out.at[t], rs2_in.at[o], rs2_send.at[t], rs2_recv.at[o], (h, dst, i))

    def home_step(t, acc_b):
        src = lax.rem(o - t + no, no)
        rs2_out[t] = inner_sum(src).astype(jnp.bfloat16)
        rs2_copy(t).start()
        return acc_b + mm(low_all[src], rs2_out[t, 0], NN)

    acc_b = lax.fori_loop(1, no, home_step, jnp.zeros(gb_ref.shape, jnp.float32))
    acc = inner_sum(o)
    acc_b = acc_b + mm(low_all[o], acc[0].astype(jnp.bfloat16), NN)
    part_b[o] = (acc_b * scaling).astype(jnp.bfloat16)

    def pa_copy(t):
        return remote(part_a.at[o], part_a.at[o], pa_send.at[t], pa_recv.at[o],
                      (h, at_outer(t), i))

    def pb_copy(t):
        return remote(part_b.at[o], part_b.at[o], pb_send.at[t], pb_recv.at[o],
                      (h, at_outer(t), i))

    for t in range(1, no):
        pb_copy(t).start()

    back = jnp.zeros((ga_ref.shape[0], rows), jnp.float32)
    for t in range(1, plane):
        p = at_plane(t)
        remote(back_in.at[p], back_in.at[p], back_send.at[t], back_recv.at[p],
               plane_dev(p)).wait_recv()
    for p in range(plane):
        back = back + back_in[p].astype(jnp.float32)
    part_a[o] = mm(back.astype(jnp.bfloat16), hid_ref[...], NN).astype(jnp.bfloat16)
    for t in range(1, no):
        pa_copy(t).start()

    for t in range(1, no):
        src = at_outer(t)
        remote(rs2_out.at[t], rs2_in.at[src], rs2_send.at[t], rs2_recv.at[src],
               (h, src, i)).wait_recv()
        acc = acc + rs2_in[src].astype(jnp.float32)
    fin[i, 0] = (acc[0] * scaling).astype(jnp.bfloat16)
    fin[i, 1] = acc[1].astype(jnp.bfloat16)

    def fin_copy(k):
        return remote(fin.at[i], fin.at[i], fin_send.at[k], fin_recv.at[i], (h, o, at_inner(k)))

    def gbq_copy(k):
        return remote(gbq.at[i], gbq.at[i], gbq_send.at[k], gbq_recv.at[i], (h, o, at_inner(k)))

    for k in range(1, ni):
        fin_copy(k).start()

    for t in range(1, no):
        src = at_outer(t)
        remote(part_b.at[src], part_b.at[src], pb_send.at[t], pb_recv.at[src],
               (h, src, i)).wait_recv()
    total_b = part_b[0].astype(jnp.float32)
    for src in range(1, no):
        total_b += part_b[src].astype(jnp.float32)
    gbq[i] = total_b
    for k in range(1, ni):
        gbq_copy(k).start()

    for k in range(1, ni):
        j = at_inner(k)
        remote(fin.at[j], fin.at[j], fin_send.at[k], fin_recv.at[j], (h, o, j)).wait_recv()
    dk_ref[...] = fin[:, 0].reshape(rows, HEAD_DIM)
    dv_ref[...] = fin[:, 1].reshape(rows, HEAD_DIM)
    for k in range(1, ni):
        j = at_inner(k)
        remote(gbq.at[j], gbq.at[j], gbq_send.at[k], gbq_recv.at[j], (h, o, j)).wait_recv()
    total_b = gbq[0]
    for j in range(1, ni):
        total_b = total_b + gbq[j]
    gb_ref[...] = total_b

    for t in range(1, no):
        kv_copy(t).wait_send()
        rs2_copy(t).wait_send()
        zb_copy(t).wait_send()
        la_copy(t).wait_send()
        for k in range(ni // 2):
            if k:
                cross_copy(lax.rem(o - t + no, no), t, k).wait_send()
            sibling_copy(lax.rem(o - t + no, no), t, k).wait_send()
    for t in range(1, plane):
        low_copy(t).wait_send()
        back_copy(t).wait_send()
    for src in range(no):
        for k in range(1, ni):
            rs1_copy(src, k).wait_send()
    for k in range(1, ni):
        fin_copy(k).wait_send()
        gbq_copy(k).wait_send()

    for t in range(1, no):
        src = at_outer(t)
        remote(part_a.at[src], part_a.at[src], pa_send.at[t], pa_recv.at[src],
               (h, src, i)).wait_recv()
    total_a = part_a[0].astype(jnp.float32)
    for src in range(1, no):
        total_a += part_a[src].astype(jnp.float32)
    ga_ref[...] = total_a
    for t in range(1, no):
        pa_copy(t).wait_send()
        pb_copy(t).wait_send()


def put_out(*refs):
    count = len(refs) // 2
    sem = refs[-1]
    copies = [
        pltpu.make_async_copy(refs[n], refs[count + n], sem.at[n]) for n in range(count)
    ]
    for copy in copies:
        copy.start()
    for copy in copies:
        copy.wait()


def on_device(
    sizes, queries, keys, values, grad_out, hidden_in, adapter_a, adapter_b, block_order, doc_ids
):
    nh, no, ni = sizes
    rows = queries.shape[0]
    half = rows // 2
    part = rows // ni
    width = hidden_in.shape[1]
    rank = adapter_a.shape[1]
    heads = queries.shape[1] // HEAD_DIM
    plane = nh * ni
    docs = doc_ids.reshape(-1, half)
    bf, f32 = jnp.bfloat16, jnp.float32
    dma = pltpu.SemaphoreType.DMA
    vmem = pl.BlockSpec(memory_space=pltpu.VMEM)
    hbm = pl.BlockSpec(memory_space=pl.ANY)
    share = (2, part, HEAD_DIM)
    results = (
        (queries.shape, bf),
        (keys.shape, bf),
        (values.shape, bf),
        ((rank, width), f32),
        ((rank, HEAD_DIM), f32),
    )
    held = pl.pallas_call(
        functools.partial(kernel, (nh, no, ni, heads)),
        out_shape=tuple(pltpu.VMEM(*result) for result in results),
        in_specs=[
            pl.BlockSpec(memory_space=pltpu.SMEM), vmem, hbm, hbm, hbm, hbm, hbm, vmem, vmem,
        ],
        out_specs=(vmem,) * 5,
        scratch_shapes=[
            pltpu.VMEM(queries.shape, bf),
            pltpu.VMEM(queries.shape, bf),
            pltpu.VMEM((rows, width), bf),
            pltpu.VMEM((no, ni) + share, bf),
            pltpu.VMEM((no, heads, rows, rows), f32),
            pltpu.VMEM((no, heads, rows, rows), f32),
            pltpu.VMEM(queries.shape, f32),
            pltpu.VMEM((ni, rank, part), f32),
            pltpu.VMEM((plane, rank, part), f32),
            pltpu.VMEM((no, rank, part), bf),
            pltpu.VMEM((no, ni) + share, bf),
            pltpu.VMEM((no, ni) + share, bf),
            pltpu.VMEM((no,) + share, bf),
            pltpu.VMEM((no,) + share, bf),
            pltpu.VMEM((ni,) + share, bf),
            pltpu.VMEM((ni, rank, HEAD_DIM), f32),
            pltpu.VMEM((no, rank, rows), bf),
            pltpu.VMEM((no, rank, rows), bf),
            pltpu.VMEM((plane, rank, rows), bf),
            pltpu.VMEM((no, rank, width), bf),
            pltpu.VMEM((no, rank, HEAD_DIM), bf),
            dma((3 + 2 * ni,)),
            dma((no,)), dma((no, ni)), dma((no, ni // 2)), dma((no, ni // 2)),
            dma((plane,)), dma((plane,)), dma((no,)), dma((no,)),
            dma((no, ni)), dma((no, ni)),
            dma((no,)), dma((no,)),
            dma((ni,)), dma((ni,)),
            dma((ni,)), dma((ni,)), dma((no,)), dma((no,)),
            dma((plane,)), dma((plane,)),
            dma((no,)), dma((no,)),
            dma((no,)), dma((no,)),
        ],
        compiler_params=pltpu.CompilerParams(
            collective_id=0, has_side_effects=True, vmem_limit_bytes=60 * 1024 * 1024
        ),
    )(block_order, docs, queries, keys, values, grad_out, hidden_in, adapter_a.T, adapter_b)
    grad_query, grad_key, grad_value, grad_a, grad_b = pl.pallas_call(
        put_out,
        out_shape=tuple(jax.ShapeDtypeStruct(*result) for result in results),
        in_specs=[vmem] * len(results),
        out_specs=(hbm,) * len(results),
        scratch_shapes=[dma((len(results),))],
        compiler_params=pltpu.CompilerParams(vmem_limit_bytes=8 * 1024 * 1024),
    )(*held)
    return grad_query, grad_key, grad_value, grad_a.T, grad_b


def solution(mesh):
    sizes = tuple(mesh.shape[name] for name in ("head", "outer", "inner"))
    in_specs = (
        P("outer", ("head", "inner")),
        P("outer", "head"),
        P("outer", "head"),
        P("outer", ("head", "inner")),
        P("outer", ("head", "inner")),
        P(("head", "inner"), None),
        P(None, "head"),
        P(),
        P(),
    )
    out_specs = (
        P("outer", ("head", "inner")),
        P("outer", "head"),
        P("outer", "head"),
        P(("head", "inner"), None),
        P(None, "head"),
    )
    return jax.shard_map(
        functools.partial(on_device, sizes),
        mesh=mesh, in_specs=in_specs, out_specs=out_specs, check_vma=False,
    )
```

```python
import functools

import jax
import jax.numpy as jnp
from jax import lax
from jax.experimental import pallas as pl
from jax.experimental.pallas import tpu as pltpu
from jax.sharding import PartitionSpec as P

HEAD_DIM = 128
NEGATIVE = -1e30
MESH = pl.DeviceIdType.MESH
NT = (((1,), (1,)), ((), ()))
NN = (((1,), (0,)), ((), ()))
TN = (((0,), (0,)), ((), ()))


def mm(a, b, dims):
    return lax.dot_general(a, b, dims, preferred_element_type=jnp.float32)


def kernel(
    sizes,
    order_ref, docs_ref, q_hbm, k_hbm, v_hbm, g_hbm, hid_hbm, at_ref, b_ref,
    dq_ref, dk_ref, dv_ref, ga_ref, gb_ref,
    q_ref, g_ref, hid_ref, kv, st, dpt, dq_acc,
    low_out, low_in, low_all, rs1_out, rs1_in, rsx_out, rsx_in, rs2_out, rs2_in, fin, gbq, zb_out, zb_in, back_in,
    part_a, part_b,
    load_sem, kv_send, kv_recv, fx_send, fs_send, low_send, low_recv, la_send, la_recv,
    rs1_send, rs1_recv, rsx_send, rsx_recv, rs2_send, rs2_recv, fin_send, fin_recv,
    gbq_send, gbq_recv, zb_send, zb_recv, back_send, back_recv,
    pa_send, pa_recv, pb_send, pb_recv,
):
    nh, no, ni, heads = sizes
    h, o, i = lax.axis_index("head"), lax.axis_index("outer"), lax.axis_index("inner")
    rows = q_ref.shape[0]
    half = rows // 2
    part = rows // ni
    plane = nh * ni
    me = h * ni + i
    scaling = HEAD_DIM ** -0.5

    def at_outer(t):
        return lax.rem(o + t, no)

    def at_inner(t):
        return lax.rem(i + t, ni)

    def at_plane(t):
        return lax.rem(me + t, plane)

    def remote(src, dst, send, recv, dev):
        return pltpu.make_async_remote_copy(
            src_ref=src, dst_ref=dst, send_sem=send, recv_sem=recv, device_id=dev,
            device_id_type=MESH,
        )

    def plane_dev(p):
        return (p // ni, o, lax.rem(p, ni))

    kv_loads = []
    for j in range(ni):
        for which, src in enumerate((k_hbm, v_hbm)):
            kv_loads.append(
                pltpu.make_async_copy(
                    src.at[pl.ds(j * part, part)], kv.at[o, j, which],
                    load_sem.at[3 + 2 * j + which],
                )
            )
    q_load = pltpu.make_async_copy(q_hbm, q_ref, load_sem.at[0])
    g_load = pltpu.make_async_copy(g_hbm, g_ref, load_sem.at[1])
    hid_load = pltpu.make_async_copy(hid_hbm, hid_ref, load_sem.at[2])
    for copy in kv_loads + [hid_load, q_load, g_load]:
        copy.start()

    barrier = pltpu.get_barrier_semaphore()
    for t in range(1, no):
        pl.semaphore_signal(barrier, inc=1, device_id=(h, at_outer(t), i), device_id_type=MESH)
    for t in range(1, plane):
        pl.semaphore_signal(barrier, inc=1, device_id=plane_dev(at_plane(t)), device_id_type=MESH)
    pl.semaphore_wait(barrier, no - 1 + plane - 1)

    for copy in kv_loads:
        copy.wait()

    def kv_copy(t):
        return remote(kv.at[o, i], kv.at[o, i], kv_send.at[t], kv_recv.at[o, i],
                      (h, at_outer(t), i))

    def slot_wait(src, j):
        remote(kv.at[src, j], kv.at[src, j], kv_send.at[0], kv_recv.at[src, j],
               (h, at_outer(1), i)).wait_recv()

    sibling = i + 1 - 2 * lax.rem(i, 2)

    def cross(k):
        return at_inner(2 * k)

    def cross_copy(src, t, k):
        return remote(kv.at[src, i], kv.at[src, i], fx_send.at[t, k], kv_recv.at[src, i],
                      (h, o, cross(k)))

    def sibling_copy(src, t, k):
        j = cross(k)
        return remote(kv.at[src, j], kv.at[src, j], fs_send.at[t, k], kv_recv.at[src, j],
                      (h, o, sibling))

    for t in range(1, no):
        kv_copy(t).start()

    hid_load.wait()
    for j in range(ni):
        low_out[j] = mm(at_ref[...], hid_ref[j * part:(j + 1) * part, :], NT)
    low_in[me] = low_out[i]

    def low_copy(t):
        p = at_plane(t)
        return remote(low_out.at[lax.rem(p, ni)], low_in.at[me], low_send.at[t],
                      low_recv.at[me], plane_dev(p))

    for t in range(1, plane):
        low_copy(t).start()

    q_load.wait()
    g_load.wait()

    def row_meta(block):
        idx = order_ref[block]
        doc = docs_ref[pl.ds(idx, 1), :].astype(jnp.float32)
        return doc, idx * half

    lanes = lax.broadcasted_iota(jnp.int32, (1, half), 1)
    sublanes = lax.broadcasted_iota(jnp.int32, (half, rows), 0)
    qm = [row_meta(2 * o + b) for b in range(2)]
    q_doc = jnp.concatenate([m[0] for m in qm], 1)
    q_pos = jnp.concatenate([m[1] + lanes for m in qm], 1)

    def head_cols(x):
        return slice(x * HEAD_DIM, (x + 1) * HEAD_DIM)

    def block_scores(src, t, peaks):
        key_rows = kv[src, :, 0].reshape(rows, HEAD_DIM)
        val_rows = kv[src, :, 1].reshape(rows, HEAD_DIM)
        docs, poss = [], []
        for b in range(2):
            doc, first = row_meta(2 * src + b)
            wide = jnp.transpose(jnp.broadcast_to(doc, (half, half)))
            docs.append(jnp.concatenate([wide] * (rows // half), 1))
            poss.append(first + sublanes)
        seen = (jnp.concatenate(docs, 0) == q_doc) & (jnp.concatenate(poss, 0) <= q_pos)
        out = []
        for x in range(heads):
            s = mm(key_rows, q_ref[:, head_cols(x)], NT) * scaling
            s = jnp.where(seen, s, NEGATIVE)
            st[t, x] = s
            out.append(jnp.maximum(peaks[x], jnp.max(s, axis=0, keepdims=True)))
            dpt[t, x] = mm(val_rows, g_ref[:, head_cols(x)], NT)
        return tuple(out)

    peaks = tuple(jnp.full((1, rows), NEGATIVE, jnp.float32) for _ in range(heads))
    peaks = block_scores(o, 0, peaks)

    def forward(t):
        src = lax.rem(o - t + no, no)
        slot_wait(src, i)
        for k in range(1, ni // 2):
            cross_copy(src, t, k).start()
        sibling_copy(src, t, 0).start()

    forward(1)

    def gather_step(t, peaks):
        @pl.when(t < no - 1)
        def _():
            forward(t + 1)

        src = lax.rem(o - t + no, no)
        for k in range(1, ni // 2):
            slot_wait(src, cross(k))
            sibling_copy(src, t, k).start()
        for k in range(ni // 2):
            slot_wait(src, lax.rem(sibling + 2 * k, ni))
        return block_scores(src, t, peaks)

    peaks = lax.fori_loop(1, no, gather_step, peaks)

    low = low_in[me]
    for t in range(1, plane):
        p = at_plane(t)
        remote(low_out.at[0], low_in.at[p], low_send.at[t], low_recv.at[p],
               plane_dev(p)).wait_recv()
        low = low + low_in[p]
    low_all[o] = low.astype(jnp.bfloat16)

    def la_copy(t):
        return remote(low_all.at[o], low_all.at[o], la_send.at[t], la_recv.at[o],
                      (h, at_outer(t), i))

    for t in range(1, no):
        la_copy(t).start()

    zero = jnp.zeros((1, rows), jnp.float32)

    def weigh_step(t, carried):
        out = []
        for x in range(heads):
            total, dot = carried[x]
            w = jnp.exp(st[t, x] - peaks[x])
            st[t, x] = w
            out.append((total + jnp.sum(w, axis=0, keepdims=True),
                        dot + jnp.sum(w * dpt[t, x], axis=0, keepdims=True)))
        return tuple(out)

    sums = lax.fori_loop(0, no, weigh_step, tuple((zero, zero) for _ in range(heads)))
    inv = [1.0 / total for total, _ in sums]
    delta = [dot * r for (_, dot), r in zip(sums, inv)]

    dq_acc[...] = jnp.zeros_like(dq_acc)

    def rs1_copy(src, k):
        j = lax.rem(sibling + 2 * k, ni)
        return remote(rs1_out.at[src, j], rs1_in.at[src, j], rs1_send.at[src, k],
                      rs1_recv.at[src, j], (h, o, sibling))

    def rsx_copy(src, k):
        return remote(rsx_out.at[src, k], rsx_in.at[src, i], rsx_send.at[src, k],
                      rsx_recv.at[src, i], (h, o, cross(k)))

    def pair_step(src):
        for k in reversed(range(ni // 2)):
            j = cross(k)
            remote(rs1_out.at[src, j], rs1_in.at[src, j], rs1_send.at[src, k],
                   rs1_recv.at[src, j], (h, o, sibling)).wait_recv()
            if k:
                pair = rs1_out[src, j].astype(jnp.float32) + rs1_in[src, j].astype(jnp.float32)
                rsx_out[src, k] = pair.astype(jnp.bfloat16)
                rsx_copy(src, k).start()

    def zb_copy(t):
        dst = lax.rem(o - t + no, no)
        return remote(zb_out.at[t], zb_in.at[o], zb_send.at[t], zb_recv.at[o], (h, dst, i))

    def grad_step(n, _):
        t = lax.rem(n + 1, no)
        src = lax.rem(o - t + no, no)
        key_rows = kv[src, :, 0].reshape(rows, HEAD_DIM)
        dk = jnp.zeros((rows, HEAD_DIM), jnp.float32)
        dv = jnp.zeros((rows, HEAD_DIM), jnp.float32)
        for x in range(heads):
            p = st[t, x] * inv[x]
            ds = (p * (dpt[t, x] - delta[x])).astype(jnp.bfloat16)
            dv += mm(p.astype(jnp.bfloat16), g_ref[:, head_cols(x)], NN)
            dk += mm(ds, q_ref[:, head_cols(x)], NN)
            dq_acc[:, head_cols(x)] += mm(ds, key_rows, TN)
        rs1_out[src, :, 0] = dk.astype(jnp.bfloat16).reshape(ni, part, HEAD_DIM)
        rs1_out[src, :, 1] = dv.astype(jnp.bfloat16).reshape(ni, part, HEAD_DIM)
        for k in reversed(range(ni // 2)):
            rs1_copy(src, k).start()
        back = mm(b_ref[...], dk.astype(jnp.bfloat16), NT) * scaling
        zb_out[t] = back.astype(jnp.bfloat16)

        @pl.when(t > 0)
        def _():
            zb_copy(t).start()

        @pl.when(n > 0)
        def _():
            pair_step(lax.rem(o - n + no, no))

        return 0

    lax.fori_loop(0, no, grad_step, 0)
    pair_step(o)
    dq_ref[...] = (dq_acc[...] * scaling).astype(jnp.bfloat16)

    acc = zb_out[0].astype(jnp.float32)
    for t in range(1, no):
        src = at_outer(t)
        remote(zb_out.at[t], zb_in.at[src], zb_send.at[t], zb_recv.at[src],
               (h, src, i)).wait_recv()
        acc = acc + zb_in[src].astype(jnp.float32)
    back_in[me] = acc.astype(jnp.bfloat16)

    def back_copy(t):
        return remote(back_in.at[me], back_in.at[me], back_send.at[t], back_recv.at[me],
                      plane_dev(at_plane(t)))

    for t in range(1, plane):
        back_copy(t).start()

    for t in range(1, no):
        src = at_outer(t)
        remote(low_all.at[src], low_all.at[src], la_send.at[t], la_recv.at[src],
               (h, src, i)).wait_recv()

    def inner_sum(src):
        acc = rs1_out[src, i].astype(jnp.float32) + rs1_in[src, i].astype(jnp.float32)
        for k in range(1, ni // 2):
            j = cross(k)
            remote(rsx_out.at[src, k], rsx_in.at[src, j], rsx_send.at[src, k],
                   rsx_recv.at[src, j], (h, o, j)).wait_recv()
            acc = acc + rsx_in[src, j].astype(jnp.float32)
        return acc

    def rs2_copy(t):
        dst = lax.rem(o - t + no, no)
        return remote(rs2_out.at[t], rs2_in.at[o], rs2_send.at[t], rs2_recv.at[o], (h, dst, i))

    def home_step(t, acc_b):
        src = lax.rem(o - t + no, no)
        rs2_out[t] = inner_sum(src).astype(jnp.bfloat16)
        rs2_copy(t).start()
        return acc_b + mm(low_all[src], rs2_out[t, 0], NN)

    acc_b = lax.fori_loop(1, no, home_step, jnp.zeros(gb_ref.shape, jnp.float32))
    acc = inner_sum(o)
    acc_b = acc_b + mm(low_all[o], acc[0].astype(jnp.bfloat16), NN)
    part_b[o] = (acc_b * scaling).astype(jnp.bfloat16)

    def pa_copy(t):
        return remote(part_a.at[o], part_a.at[o], pa_send.at[t], pa_recv.at[o],
                      (h, at_outer(t), i))

    def pb_copy(t):
        return remote(part_b.at[o], part_b.at[o], pb_send.at[t], pb_recv.at[o],
                      (h, at_outer(t), i))

    for t in range(1, no):
        pb_copy(t).start()

    back = jnp.zeros((ga_ref.shape[0], rows), jnp.float32)
    for t in range(1, plane):
        p = at_plane(t)
        remote(back_in.at[p], back_in.at[p], back_send.at[t], back_recv.at[p],
               plane_dev(p)).wait_recv()
    for p in range(plane):
        back = back + back_in[p].astype(jnp.float32)
    part_a[o] = mm(back.astype(jnp.bfloat16), hid_ref[...], NN).astype(jnp.bfloat16)
    for t in range(1, no):
        pa_copy(t).start()

    for t in range(1, no):
        src = at_outer(t)
        remote(rs2_out.at[t], rs2_in.at[src], rs2_send.at[t], rs2_recv.at[src],
               (h, src, i)).wait_recv()
        acc = acc + rs2_in[src].astype(jnp.float32)
    fin[i, 0] = (acc[0] * scaling).astype(jnp.bfloat16)
    fin[i, 1] = acc[1].astype(jnp.bfloat16)

    def fin_copy(k):
        return remote(fin.at[i], fin.at[i], fin_send.at[k], fin_recv.at[i], (h, o, at_inner(k)))

    def gbq_copy(k):
        return remote(gbq.at[i], gbq.at[i], gbq_send.at[k], gbq_recv.at[i], (h, o, at_inner(k)))

    for k in range(1, ni):
        fin_copy(k).start()

    for t in range(1, no):
        src = at_outer(t)
        remote(part_b.at[src], part_b.at[src], pb_send.at[t], pb_recv.at[src],
               (h, src, i)).wait_recv()
    total_b = part_b[0].astype(jnp.float32)
    for src in range(1, no):
        total_b += part_b[src].astype(jnp.float32)
    gbq[i] = total_b
    for k in range(1, ni):
        gbq_copy(k).start()

    for k in range(1, ni):
        j = at_inner(k)
        remote(fin.at[j], fin.at[j], fin_send.at[k], fin_recv.at[j], (h, o, j)).wait_recv()
    dk_ref[...] = fin[:, 0].reshape(rows, HEAD_DIM)
    dv_ref[...] = fin[:, 1].reshape(rows, HEAD_DIM)
    for k in range(1, ni):
        j = at_inner(k)
        remote(gbq.at[j], gbq.at[j], gbq_send.at[k], gbq_recv.at[j], (h, o, j)).wait_recv()
    total_b = gbq[0]
    for j in range(1, ni):
        total_b = total_b + gbq[j]
    gb_ref[...] = total_b

    for t in range(1, no):
        kv_copy(t).wait_send()
        rs2_copy(t).wait_send()
        zb_copy(t).wait_send()
        la_copy(t).wait_send()
        for k in range(ni // 2):
            if k:
                cross_copy(lax.rem(o - t + no, no), t, k).wait_send()
            sibling_copy(lax.rem(o - t + no, no), t, k).wait_send()
    for t in range(1, plane):
        low_copy(t).wait_send()
        back_copy(t).wait_send()
    for src in range(no):
        for k in range(ni // 2):
            rs1_copy(src, k).wait_send()
            if k:
                rsx_copy(src, k).wait_send()
    for k in range(1, ni):
        fin_copy(k).wait_send()
        gbq_copy(k).wait_send()

    for t in range(1, no):
        src = at_outer(t)
        remote(part_a.at[src], part_a.at[src], pa_send.at[t], pa_recv.at[src],
               (h, src, i)).wait_recv()
    total_a = part_a[0].astype(jnp.float32)
    for src in range(1, no):
        total_a += part_a[src].astype(jnp.float32)
    ga_ref[...] = total_a
    for t in range(1, no):
        pa_copy(t).wait_send()
        pb_copy(t).wait_send()


def put_out(*refs):
    count = len(refs) // 2
    sem = refs[-1]
    copies = [
        pltpu.make_async_copy(refs[n], refs[count + n], sem.at[n]) for n in range(count)
    ]
    for copy in copies:
        copy.start()
    for copy in copies:
        copy.wait()


def on_device(
    sizes, queries, keys, values, grad_out, hidden_in, adapter_a, adapter_b, block_order, doc_ids
):
    nh, no, ni = sizes
    rows = queries.shape[0]
    half = rows // 2
    part = rows // ni
    width = hidden_in.shape[1]
    rank = adapter_a.shape[1]
    heads = queries.shape[1] // HEAD_DIM
    plane = nh * ni
    docs = doc_ids.reshape(-1, half)
    bf, f32 = jnp.bfloat16, jnp.float32
    dma = pltpu.SemaphoreType.DMA
    vmem = pl.BlockSpec(memory_space=pltpu.VMEM)
    hbm = pl.BlockSpec(memory_space=pl.ANY)
    share = (2, part, HEAD_DIM)
    results = (
        (queries.shape, bf),
        (keys.shape, bf),
        (values.shape, bf),
        ((rank, width), f32),
        ((rank, HEAD_DIM), f32),
    )
    held = pl.pallas_call(
        functools.partial(kernel, (nh, no, ni, heads)),
        out_shape=tuple(pltpu.VMEM(*result) for result in results),
        in_specs=[
            pl.BlockSpec(memory_space=pltpu.SMEM), vmem, hbm, hbm, hbm, hbm, hbm, vmem, vmem,
        ],
        out_specs=(vmem,) * 5,
        scratch_shapes=[
            pltpu.VMEM(queries.shape, bf),
            pltpu.VMEM(queries.shape, bf),
            pltpu.VMEM((rows, width), bf),
            pltpu.VMEM((no, ni) + share, bf),
            pltpu.VMEM((no, heads, rows, rows), f32),
            pltpu.VMEM((no, heads, rows, rows), f32),
            pltpu.VMEM(queries.shape, f32),
            pltpu.VMEM((ni, rank, part), f32),
            pltpu.VMEM((plane, rank, part), f32),
            pltpu.VMEM((no, rank, part), bf),
            pltpu.VMEM((no, ni) + share, bf),
            pltpu.VMEM((no, ni) + share, bf),
            pltpu.VMEM((no, ni // 2) + share, bf),
            pltpu.VMEM((no, ni) + share, bf),
            pltpu.VMEM((no,) + share, bf),
            pltpu.VMEM((no,) + share, bf),
            pltpu.VMEM((ni,) + share, bf),
            pltpu.VMEM((ni, rank, HEAD_DIM), f32),
            pltpu.VMEM((no, rank, rows), bf),
            pltpu.VMEM((no, rank, rows), bf),
            pltpu.VMEM((plane, rank, rows), bf),
            pltpu.VMEM((no, rank, width), bf),
            pltpu.VMEM((no, rank, HEAD_DIM), bf),
            dma((3 + 2 * ni,)),
            dma((no,)), dma((no, ni)), dma((no, ni // 2)), dma((no, ni // 2)),
            dma((plane,)), dma((plane,)), dma((no,)), dma((no,)),
            dma((no, ni // 2)), dma((no, ni)), dma((no, ni // 2)), dma((no, ni)),
            dma((no,)), dma((no,)),
            dma((ni,)), dma((ni,)),
            dma((ni,)), dma((ni,)), dma((no,)), dma((no,)),
            dma((plane,)), dma((plane,)),
            dma((no,)), dma((no,)),
            dma((no,)), dma((no,)),
        ],
        compiler_params=pltpu.CompilerParams(
            collective_id=0, has_side_effects=True, vmem_limit_bytes=60 * 1024 * 1024
        ),
    )(block_order, docs, queries, keys, values, grad_out, hidden_in, adapter_a.T, adapter_b)
    grad_query, grad_key, grad_value, grad_a, grad_b = pl.pallas_call(
        put_out,
        out_shape=tuple(jax.ShapeDtypeStruct(*result) for result in results),
        in_specs=[vmem] * len(results),
        out_specs=(hbm,) * len(results),
        scratch_shapes=[dma((len(results),))],
        compiler_params=pltpu.CompilerParams(vmem_limit_bytes=8 * 1024 * 1024),
    )(*held)
    return grad_query, grad_key, grad_value, grad_a.T, grad_b


def solution(mesh):
    sizes = tuple(mesh.shape[name] for name in ("head", "outer", "inner"))
    in_specs = (
        P("outer", ("head", "inner")),
        P("outer", "head"),
        P("outer", "head"),
        P("outer", ("head", "inner")),
        P("outer", ("head", "inner")),
        P(("head", "inner"), None),
        P(None, "head"),
        P(),
        P(),
    )
    out_specs = (
        P("outer", ("head", "inner")),
        P("outer", "head"),
        P("outer", "head"),
        P(("head", "inner"), None),
        P(None, "head"),
    )
    return jax.shard_map(
        functools.partial(on_device, sizes),
        mesh=mesh, in_specs=in_specs, out_specs=out_specs, check_vma=False,
    )
```
